32 devices in a mesh: row: 4 (over z), col: 8 (over y, x, core).
Axes of the slice: x: 2, y: 2, z: 4, core: 2. Of those that a mesh axis runs over, the one named last changes fastest.
Arguments:
- coefs: float32 [2, 384, 16384], P(None, 'row', 'col'), may hold values from -600 to 600, as said below
- tilts: int32 [384, 2], replicated, may hold values from 8 to 48
- start_basis: float32 [384, 32], P('col'), may hold values from -6 to 6
Outputs:
- ccc: float32 [384, 384], P('row', 'col')
- basis: float32 [384, 32], P('col')
The draws below stay inside these ranges and needn't reach their ends.
Inputs may be any that keep to these rules, and one draw needn't show every extreme that they name: `coefs`: real and imaginary parts are products of a particle scale, a coefficient scale and a bounded random value.
All inputs are finite; a program needn't handle non-finite values.
Results may differ from the reference program's by a relative error of at most 0.0003.
Values sent between devices are 32-bit elements; how exact they have to be, the bound alone decides.
A program may use at most 192 MiB of HBM per device.

```python
import math
import jax
import jax.numpy as jnp
from jax import lax

GRID = 32
K = 16384
P_SIZE = 384
EIG = 32
ITERS = 4


def draw_coefs(key, part):
    first = jax.random.fold_in(key, 11)
    second = jax.random.fold_in(key, 12)
    third = jax.random.fold_in(key, 13)
    fourth = jax.random.fold_in(key, 14)
    scale_p = jnp.exp(jax.random.uniform(first, (1, P_SIZE, 1), jnp.float32) * math.log(10.0))
    scale_k = jnp.exp(jax.random.uniform(second, (1, 1, K), jnp.float32) * math.log(10.0))
    template = jnp.clip(jax.random.normal(third, (2, 1, K), jnp.float32), -5.0, 5.0)
    noise = jnp.clip(jax.random.normal(fourth, (2, P_SIZE, K), jnp.float32), -5.0, 5.0)
    weight = 0.1
    return (scale_p * scale_k * (noise + weight * template)).astype(jnp.float32)


def plant(result, own_key, smallest, largest):
    shape = result.shape
    spot = [jax.random.randint(jax.random.fold_in(own_key, axis), (), 0, shape[axis]) for axis in range(len(shape))]
    result = result.at[tuple(spot)].set(smallest)
    longest = shape.index(max(shape))
    spot[longest] = (spot[longest] + 1) % shape[longest]
    return result.at[tuple(spot)].set(largest)


def block_scale(key, dims, shards, smallest, largest):
    def one(dim, blocks):
        draws = jax.random.uniform(jax.random.fold_in(jax.random.fold_in(key, 6), dim), (blocks,), jnp.float32, smallest / len(shards), largest / len(shards))
        return jnp.repeat(jnp.exp(draws), dims[dim] // blocks).reshape((-1,) + (1,) * (len(dims) - dim - 1))

    level = one(*shards[0])
    for cut in shards[1:]:
        level = level * one(*cut)
    return level


def gaussian(stream_key, shape, width, most, pieces=(), kind=jnp.bfloat16):
    array = jax.random.normal(stream_key, shape, jnp.float32) * width
    if len(pieces) > 0:
        array = block_scale(stream_key, shape, pieces, -0.22, 0.18) * array
    return jnp.clip(array, min=-most, max=most).astype(kind)


def setup_inputs(seed: int = 0) -> dict:
    arg_keys = jax.random.split(jax.random.key(seed), 4)
    return {
        "coefs": draw_coefs(jax.random.fold_in(arg_keys[3], 71), 0),
        "tilts": plant(jax.random.randint(arg_keys[1], (P_SIZE, 2), 8, 49), jax.random.fold_in(arg_keys[1], 1), 8, 48).astype(jnp.int32),
        "start_basis": gaussian(arg_keys[2], (P_SIZE, EIG), 1.0, 6.0, ((0, 8),), jnp.float32),
    }


EPS = 1e-06
HIGH = lax.Precision.HIGHEST

def wedge(tilt_rows, wave_index):
    wave_x = jnp.abs(wave_index // (GRID * (GRID // 2)) - GRID // 2)[None, :]
    wave_z = (wave_index % GRID - GRID // 2)[None, :]
    upward = wave_z * 16 <= tilt_rows[:, 1:2] * wave_x
    downward = -wave_z * 16 <= tilt_rows[:, 0:1] * wave_x
    return jnp.where(wave_z >= 0, upward, downward).astype(jnp.float32)

def inner(left, right):
    return lax.dot_general(left.astype(jnp.float32), right.astype(jnp.float32), (((1,), (1,)), ((), ())), precision=HIGH, preferred_element_type=jnp.float32)

def reference(coefs, tilts, start_basis):
    masks = wedge(tilts, jnp.arange(K, dtype=jnp.int32))
    paired = jnp.concatenate([coefs[0] * masks, coefs[1] * masks], axis=1)
    energy = masks * (coefs[0] * coefs[0] + coefs[1] * coefs[1])
    numer = inner(paired, paired)
    intersection = inner(energy, masks)
    ccc = numer / jnp.sqrt(intersection * intersection.T + EPS)
    current = start_basis
    for step in range(ITERS):
        wide = jnp.dot(ccc.astype(jnp.float32), current.astype(jnp.float32), precision=HIGH, preferred_element_type=jnp.float32)
        gram = lax.dot_general(wide.astype(jnp.float32), wide.astype(jnp.float32), (((0,), (0,)), ((), ())), precision=HIGH, preferred_element_type=jnp.float32)
        factor = jnp.linalg.cholesky(gram)
        current = lax.linalg.triangular_solve(factor, wide, left_side=False, lower=True, transpose_a=True)
    return (ccc, current * jnp.sqrt(jnp.float32(P_SIZE)))
```

```python
import functools
import math

import jax
import jax.numpy as jnp
from jax import lax
from jax.experimental import pallas as pl
from jax.experimental.pallas import tpu as pltpu
from jax.sharding import PartitionSpec as P

GRID = 32
ITERS = 4
EPS = 1e-06
HIGH = lax.Precision.HIGHEST
MESH = pl.DeviceIdType.MESH
TILE = 128
BLOCKS = 3


def flip(index, mask):
    out = index
    bit = 1
    while bit <= mask:
        if mask & bit:
            out = out + bit * (1 - 2 * ((index // bit) % 2))
        bit *= 2
    return out


def far_first(count):
    return sorted(range(1, count), key=lambda mask: (-mask.bit_length(), mask))


def split(value):
    high = value.astype(jnp.bfloat16)
    low = (value - high.astype(jnp.float32)).astype(jnp.bfloat16)
    return high, low


def thirds(value):
    high = value.astype(jnp.bfloat16)
    rest = value - high.astype(jnp.float32)
    middle, low = split(rest)
    return high, middle, low


def nt(left, right, precision=None):
    return lax.dot_general(
        left, right, (((1,), (1,)), ((), ())), precision=precision, preferred_element_type=jnp.float32
    )


def nn(left, right, precision=None):
    return lax.dot_general(
        left, right, (((1,), (0,)), ((), ())), precision=precision, preferred_element_type=jnp.float32
    )


def nn_six(left, right):
    lh, lm, ll = thirds(left)
    rh, rm, rl = thirds(right)
    small = nn(lm, rm) + nn(lh, rl) + nn(ll, rh)
    return nn(lh, rh) + (nn(lh, rm) + nn(lm, rh) + small)


def inverse_factor(gram):
    n = gram.shape[0]
    rows = lax.broadcasted_iota(jnp.int32, (n, n), 0)
    cols = lax.broadcasted_iota(jnp.int32, (n, n), 1)
    work = gram
    inverse = jnp.where(rows == cols, 1.0, 0.0).astype(jnp.float32)
    pivots = jnp.ones((n, n), jnp.float32)
    for j in range(n):
        column = jnp.broadcast_to(work[:, j : j + 1], (n, n))
        pivot = column[j : j + 1, :]
        reciprocal = 1.0 / pivot
        pivots = jnp.where(rows == j, pivot, pivots)
        factor = jnp.where(rows > j, column, 0.0)
        inverse = inverse - factor * (inverse[j : j + 1, :] * reciprocal)
        if j < n - 1:
            work = work - factor * (work[j : j + 1, :] * reciprocal)
    return inverse / jnp.sqrt(pivots)


def kernel(
    row_size, col_size, coefs_ref, tilts_ref, basis_ref, ccc_ref, out_ref,
    xall, start, xh, xl, eh, el, mb, part, rx_pair, rx_plane, rx_row, packed, ch, cl,
    own_sem, x_send, x_recv, v_send, v_recv, pair_send, pair_recv, plane_send, plane_recv,
    row_send, row_recv, zg_send, zg_recv, cg_send, cg_recv,
):
    z = lax.axis_index("row")
    c = lax.axis_index("col")
    rows = coefs_ref.shape[1]
    width = coefs_ref.shape[2]
    total = rows * row_size
    piece = width // row_size
    basis_rows = basis_ref.shape[0]
    size = total // BLOCKS

    barrier = pltpu.get_barrier_semaphore()
    for mask in range(1, row_size):
        pl.semaphore_signal(barrier, inc=1, device_id={"row": flip(z, mask)}, device_id_type=MESH)
    for mask in range(1, col_size):
        pl.semaphore_signal(barrier, inc=1, device_id={"col": flip(c, mask)}, device_id_type=MESH)
    pl.semaphore_wait(barrier, row_size + col_size - 2)

    def remote(source, target, send, recv, mask, axis):
        other = flip(z if axis == "row" else c, mask)
        return pltpu.make_async_remote_copy(
            src_ref=source, dst_ref=target, send_sem=send.at[mask - 1], recv_sem=recv.at[mask - 1],
            device_id={axis: other}, device_id_type=MESH,
        )

    own_rows = pl.ds(pl.multiple_of(z * rows, 8), rows)
    exchange = {}
    for mask in far_first(row_size):
        lanes = pl.ds(pl.multiple_of(flip(z, mask) * piece, TILE), piece)
        exchange[mask] = remote(coefs_ref.at[:, :, lanes], xall.at[:, own_rows, :], x_send, x_recv, mask, "row")
        exchange[mask].start()
    own = pltpu.make_async_copy(
        coefs_ref.at[:, :, pl.ds(pl.multiple_of(z * piece, TILE), piece)], xall.at[:, own_rows, :], own_sem
    )
    own.start()
    start_rows = pl.ds(pl.multiple_of(c * basis_rows, 8), basis_rows)
    start[start_rows, :] = basis_ref[...]
    starts = []
    for mask in range(1, col_size):
        copy = remote(basis_ref, start.at[start_rows, :], v_send, v_recv, mask, "col")
        copy.start()
        starts.append(copy)

    wave = c * width + z * piece + lax.broadcasted_iota(jnp.int32, (1, piece), 1)
    wave_x = jnp.abs(wave // (GRID * (GRID // 2)) - GRID // 2)
    wave_z = wave % GRID - GRID // 2

    def prepare(index):
        span = pl.ds(pl.multiple_of(index * rows, 16), rows)
        tilt = tilts_ref[span, :]
        upward = wave_z * 16 <= tilt[:, 1:2] * wave_x
        downward = -wave_z * 16 <= tilt[:, 0:1] * wave_x
        mask = jnp.where(jnp.logical_or(jnp.logical_and(wave_z >= 0, upward), jnp.logical_and(wave_z < 0, downward)), 1.0, 0.0)
        mb[span, :] = mask.astype(jnp.bfloat16)
        real = xall[0, span, :] * mask
        imag = xall[1, span, :] * mask
        xh[span, :piece], xl[span, :piece] = split(real)
        xh[span, piece:], xl[span, piece:] = split(imag)
        eh[span, :], el[span, :] = split(real * real + imag * imag)

    own.wait()
    prepare(z)
    for mask in reversed(far_first(row_size)):
        exchange[mask].wait()
        prepare(flip(z, mask))

    for a in range(BLOCKS):
        for t in range(2):
            b = (a + t) % BLOCKS
            right = slice(b * size, (b + 1) * size)
            lanes = slice(t * size, (t + 1) * size)

            def tile(index, carry, a=a, right=right, lanes=lanes):
                left = pl.ds(pl.multiple_of(a * size + index * TILE, TILE), TILE)
                part[0, left, lanes] = (
                    nt(xh[left, :], xh[right, :]) + nt(xh[left, :], xl[right, :]) + nt(xl[left, :], xh[right, :])
                )
                part[1, left, lanes] = nt(eh[left, :], mb[right, :]) + nt(el[left, :], mb[right, :])
                part[2, left, lanes] = nt(mb[left, :], eh[right, :]) + nt(mb[left, :], el[right, :])
                return carry

            lax.fori_loop(0, size // TILE, tile, 0)

    pairs = col_size // 2
    side = c % 2
    half = total // 2
    strip = total // col_size
    theirs = pl.ds(pl.multiple_of((1 - side) * half, 8), half)
    mine = pl.ds(pl.multiple_of(side * half, 8), half)
    pair = remote(part.at[:, theirs, :], rx_pair, pair_send, pair_recv, 1, "col")
    pair.start()
    pair.wait()
    part[:, mine, :] = part[:, mine, :] + rx_pair[...]
    group = c // 2
    copies = []
    for mask in far_first(pairs):
        there = pl.ds(pl.multiple_of(side * half + flip(group, mask) * strip, 8), strip)
        copy = pltpu.make_async_remote_copy(
            src_ref=part.at[:, there, :], dst_ref=rx_plane.at[mask - 1],
            send_sem=plane_send.at[mask - 1], recv_sem=plane_recv.at[mask - 1],
            device_id={"col": flip(c, 2 * mask)}, device_id_type=MESH,
        )
        copy.start()
        copies.append(copy)
    for copy in copies:
        copy.wait()
    base = side * half + group * strip
    strip_rows = pl.ds(pl.multiple_of(base, 8), strip)
    part[:, strip_rows, :] = part[:, strip_rows, :] + sum(rx_plane[k] for k in range(pairs - 1))

    cuts = row_size // 2
    short = strip // cuts

    def region(index):
        return (
            pl.ds(pl.multiple_of(base + (index // 2) * short, 8), short),
            pl.ds(pl.multiple_of((index % 2) * size, TILE), size),
        )

    copies = []
    for mask in far_first(row_size):
        there = region(flip(z, mask))
        copy = remote(part.at[:, there[0], there[1]], rx_row.at[mask - 1], row_send, row_recv, mask, "row")
        copy.start()
        copies.append(copy)
    for copy in copies:
        copy.wait()
    here = region(z)
    sums = part[:, here[0], here[1]] + sum(rx_row[k] for k in range(row_size - 1))
    packed[here[0], here[1]] = sums[0] / jnp.sqrt(sums[1] * sums[2] + EPS)

    copies = []
    for mask in far_first(row_size):
        spot = packed.at[here[0], here[1]]
        copy = remote(spot, spot, zg_send, zg_recv, mask, "row")
        copy.start()
        copies.append(copy)
    for copy in copies:
        copy.wait()
    copies = []
    for mask in far_first(col_size):
        spot = packed.at[strip_rows, :]
        copy = remote(spot, spot, cg_send, cg_recv, mask, "col")
        copy.start()
        copies.append(copy)
    for copy in copies:
        copy.wait()

    def place(i, j, value):
        down, across = slice(i, i + TILE), slice(j, j + TILE)
        plane, lane = (0, j) if j < 2 * size else (1, j - 2 * size)
        part[plane, down, lane : lane + TILE] = value
        ch[down, across], cl[down, across] = split(value)

    for a in range(BLOCKS):
        for t in range(2):
            b = (a + t) % BLOCKS
            for i in range(0, size, TILE):
                for j in range(0, size, TILE):
                    block = packed[a * size + i : a * size + i + TILE, t * size + j : t * size + j + TILE]
                    place(a * size + i, b * size + j, block)
                    if t:
                        place(b * size + j, a * size + i, block.T)

    chosen = lax.broadcasted_iota(jnp.int32, (basis_rows, total), 1)
    chosen = chosen == c * basis_rows + lax.broadcasted_iota(jnp.int32, (basis_rows, total), 0)
    chosen = jnp.where(chosen, 1.0, 0.0).astype(jnp.float32)
    ccc_ref[...] = nt(part[0, own_rows, :], chosen[:, : 2 * size], HIGH) + nt(
        part[1, own_rows, :size], chosen[:, 2 * size :], HIGH
    )

    for copy in starts:
        copy.wait()
    eig = basis_ref.shape[1]
    unit = lax.broadcasted_iota(jnp.int32, (eig, eig), 0) == lax.broadcasted_iota(jnp.int32, (eig, eig), 1)
    first = nt(jnp.where(unit, 1.0, 0.0).astype(jnp.float32), start[...], HIGH)

    def iterate(step, current):
        high, low = split(current)
        wide = nn(high, ch[...]) + nn(high, cl[...]) + nn(low, ch[...])
        return nn_six(inverse_factor(nt(wide, wide, HIGH)), wide)

    last = first
    for step in range(ITERS):
        last = iterate(step, last)
    out_ref[...] = nt(chosen, last, HIGH) * math.sqrt(total)


def local(coefs, tilts, start_basis):
    row_size = lax.axis_size("row")
    col_size = lax.axis_size("col")
    rows, width = coefs.shape[1:]
    basis_rows, eig = start_basis.shape
    total = rows * row_size
    piece = width // row_size
    lanes = 2 * (total // BLOCKS)
    strip = total // col_size
    pairs = col_size // 2
    f32, b16 = jnp.float32, jnp.bfloat16
    dma = lambda n: pltpu.SemaphoreType.DMA((n,))
    vmem = pl.BlockSpec(memory_space=pltpu.VMEM)
    ccc, basis = pl.pallas_call(
        functools.partial(kernel, row_size, col_size),
        out_shape=(
            jax.ShapeDtypeStruct((rows, basis_rows), f32),
            jax.ShapeDtypeStruct((basis_rows, eig), f32),
        ),
        in_specs=[pl.BlockSpec(memory_space=pl.ANY), vmem, vmem],
        out_specs=(vmem, vmem),
        scratch_shapes=[
            pltpu.VMEM((2, total, piece), f32),
            pltpu.VMEM((total, eig), f32),
            pltpu.VMEM((total, 2 * piece), b16),
            pltpu.VMEM((total, 2 * piece), b16),
            pltpu.VMEM((total, piece), b16),
            pltpu.VMEM((total, piece), b16),
            pltpu.VMEM((total, piece), b16),
            pltpu.VMEM((3, total, lanes), f32),
            pltpu.VMEM((3, total // 2, lanes), f32),
            pltpu.VMEM((pairs - 1, 3, strip, lanes), f32),
            pltpu.VMEM((row_size - 1, 3, strip // (row_size // 2), lanes // 2), f32),
            pltpu.VMEM((total, lanes), f32),
            pltpu.VMEM((total, total), b16),
            pltpu.VMEM((total, total), b16),
            pltpu.SemaphoreType.DMA,
            dma(row_size - 1), dma(row_size - 1),
            dma(col_size - 1), dma(col_size - 1),
            dma(1), dma(1),
            dma(pairs - 1), dma(pairs - 1),
            dma(row_size - 1), dma(row_size - 1),
            dma(row_size - 1), dma(row_size - 1),
            dma(col_size - 1), dma(col_size - 1),
        ],
        compiler_params=pltpu.CompilerParams(
            collective_id=0, has_side_effects=True, vmem_limit_bytes=67043328
        ),
        name="subspace",
    )(coefs, tilts, start_basis)
    return ccc, basis


def solution(mesh):
    in_specs = (P(None, "row", "col"), P(), P("col", None))
    out_specs = (P("row", "col"), P("col", None))
    return jax.shard_map(local, mesh=mesh, in_specs=in_specs, out_specs=out_specs, check_vma=False)
```

```python
import functools
import math

import jax
import jax.numpy as jnp
from jax import lax
from jax.experimental import pallas as pl
from jax.experimental.pallas import tpu as pltpu
from jax.sharding import PartitionSpec as P

GRID = 32
ITERS = 4
EPS = 1e-06
HIGH = lax.Precision.HIGHEST
MESH = pl.DeviceIdType.MESH
TILE = 128
BLOCKS = 3


def flip(index, mask):
    out = index
    bit = 1
    while bit <= mask:
        if mask & bit:
            out = out + bit * (1 - 2 * ((index // bit) % 2))
        bit *= 2
    return out


def far_first(count):
    return sorted(range(1, count), key=lambda mask: (-mask.bit_length(), mask))


def split(value):
    high = value.astype(jnp.bfloat16)
    low = (value - high.astype(jnp.float32)).astype(jnp.bfloat16)
    return high, low


def thirds(value):
    high = value.astype(jnp.bfloat16)
    rest = value - high.astype(jnp.float32)
    middle, low = split(rest)
    return high, middle, low


def nt(left, right, precision=None):
    return lax.dot_general(
        left, right, (((1,), (1,)), ((), ())), precision=precision, preferred_element_type=jnp.float32
    )


def nn(left, right, precision=None):
    return lax.dot_general(
        left, right, (((1,), (0,)), ((), ())), precision=precision, preferred_element_type=jnp.float32
    )


def nn_six(left, right):
    lh, lm, ll = thirds(left)
    rh, rm, rl = thirds(right)
    small = nn(lm, rm) + nn(lh, rl) + nn(ll, rh)
    return nn(lh, rh) + (nn(lh, rm) + nn(lm, rh) + small)


def inverse_factor(gram):
    n = gram.shape[0]
    rows = lax.broadcasted_iota(jnp.int32, (n, n), 0)
    cols = lax.broadcasted_iota(jnp.int32, (n, n), 1)
    work = gram
    inverse = jnp.where(rows == cols, 1.0, 0.0).astype(jnp.float32)
    pivots = jnp.ones((n, n), jnp.float32)
    for j in range(n):
        column = jnp.broadcast_to(work[:, j : j + 1], (n, n))
        pivot = column[j : j + 1, :]
        reciprocal = 1.0 / pivot
        pivots = jnp.where(rows == j, pivot, pivots)
        factor = jnp.where(rows > j, column, 0.0)
        inverse = inverse - factor * (inverse[j : j + 1, :] * reciprocal)
        if j < n - 1:
            work = work - factor * (work[j : j + 1, :] * reciprocal)
    return inverse / jnp.sqrt(pivots)


def kernel(
    row_size, col_size, coefs_ref, tilts_ref, basis_ref, ccc_ref, out_ref,
    xall, start, first, keep, energy, xh, xl, eh, el, mb, part, rx_pair, rx_plane, rx_row, packed, ch, cl,
    own_sem, x_send, x_recv, v_send, v_recv, pair_send, pair_recv, plane_send, plane_recv,
    row_send, row_recv, zg_send, zg_recv, cg_send, cg_recv,
):
    z = lax.axis_index("row")
    c = lax.axis_index("col")
    rows = coefs_ref.shape[1]
    width = coefs_ref.shape[2]
    total = rows * row_size
    piece = width // row_size
    eig, basis_rows = basis_ref.shape
    chunks = piece // TILE
    size = total // BLOCKS

    barrier = pltpu.get_barrier_semaphore()
    for mask in range(1, row_size):
        pl.semaphore_signal(barrier, inc=1, device_id={"row": flip(z, mask)}, device_id_type=MESH)
    for mask in range(1, col_size):
        pl.semaphore_signal(barrier, inc=1, device_id={"col": flip(c, mask)}, device_id_type=MESH)
    pl.semaphore_wait(barrier, row_size + col_size - 2)

    def remote(source, target, send, recv, mask, axis):
        other = flip(z if axis == "row" else c, mask)
        return pltpu.make_async_remote_copy(
            src_ref=source, dst_ref=target, send_sem=send.at[mask - 1], recv_sem=recv.at[mask - 1],
            device_id={axis: other}, device_id_type=MESH,
        )

    own_rows = pl.ds(pl.multiple_of(z * rows, 8), rows)
    exchange = {}
    for q in range(chunks):
        here = pl.ds(q * TILE, TILE)
        for mask in far_first(row_size):
            lanes = pl.ds(pl.multiple_of(flip(z, mask) * piece + q * TILE, TILE), TILE)
            slot = q * (row_size - 1) + mask - 1
            exchange[q, mask] = pltpu.make_async_remote_copy(
                src_ref=coefs_ref.at[:, :, lanes], dst_ref=xall.at[:, own_rows, here],
                send_sem=x_send.at[slot], recv_sem=x_recv.at[slot],
                device_id={"row": flip(z, mask)}, device_id_type=MESH,
            )
            exchange[q, mask].start()
    own = pltpu.make_async_copy(
        coefs_ref.at[:, :, pl.ds(pl.multiple_of(z * piece, TILE), piece)], xall.at[:, own_rows, :], own_sem
    )
    own.start()
    start[c] = basis_ref[...]
    starts = []
    for mask in range(1, col_size):
        copy = remote(basis_ref, start.at[c], v_send, v_recv, mask, "col")
        copy.start()
        starts.append(copy)

    wave = c * width + z * piece + lax.broadcasted_iota(jnp.int32, (TILE, TILE), 1)
    wave_x = jnp.abs(wave // (GRID * (GRID // 2)) - GRID // 2).astype(jnp.float32)
    wave_z = (wave % GRID - GRID // 2).astype(jnp.float32) * 16.0
    for i in range(0, total, TILE):
        limits = tilts_ref[:, i : i + TILE].astype(jnp.float32)
        below = jnp.broadcast_to(limits[0:1, :], (TILE, TILE)).T
        above = jnp.broadcast_to(limits[1:2, :], (TILE, TILE)).T
        inside = jnp.where(wave_z >= 0, wave_z - above * wave_x, -wave_z - below * wave_x) <= 0
        mask = jnp.where(inside, 1.0, 0.0)
        keep[i : i + TILE, :] = mask
        mb[i : i + TILE, :] = mask.astype(jnp.bfloat16)

    for copy in starts:
        copy.wait()
    places = lax.broadcasted_iota(jnp.int32, (basis_rows, total), 1) - lax.broadcasted_iota(
        jnp.int32, (basis_rows, total), 0
    )
    for k in range(col_size):
        term = nn(start[k], jnp.where(places == k * basis_rows, 1.0, 0.0).astype(jnp.float32), HIGH)
        first[...] = term if k == 0 else first[...] + term

    def prepare(q, index):
        span = pl.ds(pl.multiple_of(index * rows, 16), rows)
        lanes = slice(q * TILE, (q + 1) * TILE)
        mask = keep[span, :]
        real = xall[0, span, lanes] * mask
        imag = xall[1, span, lanes] * mask
        for part_lanes, value in ((slice(2 * q * TILE, (2 * q + 1) * TILE), real), (slice((2 * q + 1) * TILE, (2 * q + 2) * TILE), imag)):
            xh[span, part_lanes], xl[span, part_lanes] = split(value)
        power = real * real + imag * imag
        if q > 0:
            power = power + energy[span, :]
        if q < chunks - 1:
            energy[span, :] = power
        else:
            eh[span, :], el[span, :] = split(power)

    def products(q):
        lanes = slice(2 * q * TILE, 2 * (q + 1) * TILE)
        for a in range(BLOCKS):
            for t in range(2):
                b = (a + t) % BLOCKS
                right = slice(b * size, (b + 1) * size)
                out = slice(t * size, (t + 1) * size)

                def tile(index, carry, a=a, right=right, out=out):
                    left = pl.ds(pl.multiple_of(a * size + index * TILE, TILE), TILE)
                    value = (
                        nt(xh[left, lanes], xh[right, lanes])
                        + nt(xh[left, lanes], xl[right, lanes])
                        + nt(xl[left, lanes], xh[right, lanes])
                    )
                    part[0, left, out] = value if q == 0 else part[0, left, out] + value
                    if q == chunks - 1:
                        part[1, left, out] = nt(eh[left, :], mb[right, :]) + nt(el[left, :], mb[right, :])
                        part[2, left, out] = nt(mb[left, :], eh[right, :]) + nt(mb[left, :], el[right, :])
                    return carry

                lax.fori_loop(0, size // TILE, tile, 0)

    own.wait()
    for q in range(chunks):
        prepare(q, z)
        for mask in far_first(row_size):
            exchange[q, mask].wait()
            prepare(q, flip(z, mask))
        products(q)

    pairs = col_size // 2
    side = c % 2
    half = total // 2
    strip = total // col_size
    theirs = pl.ds(pl.multiple_of((1 - side) * half, 8), half)
    mine = pl.ds(pl.multiple_of(side * half, 8), half)
    pair = remote(part.at[:, theirs, :], rx_pair, pair_send, pair_recv, 1, "col")
    pair.start()
    pair.wait()
    part[:, mine, :] = part[:, mine, :] + rx_pair[...]
    group = c // 2
    copies = []
    for mask in far_first(pairs):
        there = pl.ds(pl.multiple_of(side * half + flip(group, mask) * strip, 8), strip)
        copy = pltpu.make_async_remote_copy(
            src_ref=part.at[:, there, :], dst_ref=rx_plane.at[mask - 1],
            send_sem=plane_send.at[mask - 1], recv_sem=plane_recv.at[mask - 1],
            device_id={"col": flip(c, 2 * mask)}, device_id_type=MESH,
        )
        copy.start()
        copies.append(copy)
    for copy in copies:
        copy.wait()
    base = side * half + group * strip
    strip_rows = pl.ds(pl.multiple_of(base, 8), strip)
    part[:, strip_rows, :] = part[:, strip_rows, :] + sum(rx_plane[k] for k in range(pairs - 1))

    cuts = row_size // 2
    short = strip // cuts

    def region(index):
        return (
            pl.ds(pl.multiple_of(base + (index // 2) * short, 8), short),
            pl.ds(pl.multiple_of((index % 2) * size, TILE), size),
        )

    copies = []
    for mask in far_first(row_size):
        there = region(flip(z, mask))
        copy = remote(part.at[:, there[0], there[1]], rx_row.at[mask - 1], row_send, row_recv, mask, "row")
        copy.start()
        copies.append(copy)
    for copy in copies:
        copy.wait()
    here = region(z)
    sums = part[:, here[0], here[1]] + sum(rx_row[k] for k in range(row_size - 1))
    packed[here[0], here[1]] = sums[0] / jnp.sqrt(sums[1] * sums[2] + EPS)

    copies = []
    for mask in far_first(row_size):
        spot = packed.at[here[0], here[1]]
        copy = remote(spot, spot, zg_send, zg_recv, mask, "row")
        copy.start()
        copies.append(copy)
    for copy in copies:
        copy.wait()
    copies = []
    for mask in far_first(col_size):
        spot = packed.at[strip_rows, :]
        copy = remote(spot, spot, cg_send, cg_recv, mask, "col")
        copy.start()
        copies.append(copy)
    for copy in copies:
        copy.wait()

    def place(i, j, value):
        down, across = slice(i, i + TILE), slice(j, j + TILE)
        plane, lane = (0, j) if j < 2 * size else (1, j - 2 * size)
        part[plane, down, lane : lane + TILE] = value
        ch[down, across], cl[down, across] = split(value)

    for a in range(BLOCKS):
        for t in range(2):
            b = (a + t) % BLOCKS
            for i in range(0, size, TILE):
                for j in range(0, size, TILE):
                    block = packed[a * size + i : a * size + i + TILE, t * size + j : t * size + j + TILE]
                    place(a * size + i, b * size + j, block)
                    if t:
                        place(b * size + j, a * size + i, block.T)

    chosen = lax.broadcasted_iota(jnp.int32, (basis_rows, total), 1)
    chosen = chosen == c * basis_rows + lax.broadcasted_iota(jnp.int32, (basis_rows, total), 0)
    chosen = jnp.where(chosen, 1.0, 0.0).astype(jnp.float32)
    ccc_ref[...] = nt(chosen[:, : 2 * size], part[0, own_rows, :], HIGH) + nt(
        chosen[:, 2 * size :], part[1, own_rows, :size], HIGH
    )

    def iterate(step, current):
        high, low = split(current)
        wide = nn(high, ch[...]) + nn(high, cl[...]) + nn(low, ch[...])
        return nn_six(inverse_factor(nt(wide, wide, HIGH)), wide)

    last = first[...]
    for step in range(ITERS):
        last = iterate(step, last)
    out_ref[...] = nt(last, chosen, HIGH) * math.sqrt(total)


def local(coefs, tilts, start_basis):
    row_size = lax.axis_size("row")
    col_size = lax.axis_size("col")
    rows, width = coefs.shape[1:]
    basis_rows, eig = start_basis.shape
    total = rows * row_size
    piece = width // row_size
    lanes = 2 * (total // BLOCKS)
    strip = total // col_size
    pairs = col_size // 2
    f32, b16 = jnp.float32, jnp.bfloat16
    dma = lambda n: pltpu.SemaphoreType.DMA((n,))
    vmem = pl.BlockSpec(memory_space=pltpu.VMEM)
    ccc, basis = pl.pallas_call(
        functools.partial(kernel, row_size, col_size),
        out_shape=(
            jax.ShapeDtypeStruct((basis_rows, rows), f32),
            jax.ShapeDtypeStruct((eig, basis_rows), f32),
        ),
        in_specs=[pl.BlockSpec(memory_space=pl.ANY), vmem, vmem],
        out_specs=(vmem, vmem),
        scratch_shapes=[
            pltpu.VMEM((2, total, piece), f32),
            pltpu.VMEM((col_size, eig, basis_rows), f32),
            pltpu.VMEM((eig, total), f32),
            pltpu.VMEM((total, TILE), f32),
            pltpu.VMEM((total, TILE), f32),
            pltpu.VMEM((total, 2 * piece), b16),
            pltpu.VMEM((total, 2 * piece), b16),
            pltpu.VMEM((total, TILE), b16),
            pltpu.VMEM((total, TILE), b16),
            pltpu.VMEM((total, TILE), b16),
            pltpu.VMEM((3, total, lanes), f32),
            pltpu.VMEM((3, total // 2, lanes), f32),
            pltpu.VMEM((pairs - 1, 3, strip, lanes), f32),
            pltpu.VMEM((row_size - 1, 3, strip // (row_size // 2), lanes // 2), f32),
            pltpu.VMEM((total, lanes), f32),
            pltpu.VMEM((total, total), b16),
            pltpu.VMEM((total, total), b16),
            pltpu.SemaphoreType.DMA,
            dma(piece // TILE * (row_size - 1)), dma(piece // TILE * (row_size - 1)),
            dma(col_size - 1), dma(col_size - 1),
            dma(1), dma(1),
            dma(pairs - 1), dma(pairs - 1),
            dma(row_size - 1), dma(row_size - 1),
            dma(row_size - 1), dma(row_size - 1),
            dma(col_size - 1), dma(col_size - 1),
        ],
        compiler_params=pltpu.CompilerParams(
            collective_id=0, has_side_effects=True, vmem_limit_bytes=67043328
        ),
        name="subspace",
    )(coefs, tilts.T, start_basis.T)
    return ccc.T, basis.T


def solution(mesh):
    in_specs = (P(None, "row", "col"), P(), P("col", None))
    out_specs = (P("row", "col"), P("col", None))
    return jax.shard_map(local, mesh=mesh, in_specs=in_specs, out_specs=out_specs, check_vma=False)
```

```python
import functools
import math

import jax
import jax.numpy as jnp
from jax import lax
from jax.experimental import pallas as pl
from jax.experimental.pallas import tpu as pltpu
from jax.sharding import PartitionSpec as P

GRID = 32
ITERS = 4
EPS = 1e-06
HIGH = lax.Precision.HIGHEST
MESH = pl.DeviceIdType.MESH
TILE = 128
BLOCKS = 3
GROUP = 8


def flip(index, mask):
    out = index
    bit = 1
    while bit <= mask:
        if mask & bit:
            out = out + bit * (1 - 2 * ((index // bit) % 2))
        bit *= 2
    return out


def far_first(count):
    return sorted(range(1, count), key=lambda mask: (-mask.bit_length(), mask))


def split(value):
    high = value.astype(jnp.bfloat16)
    low = (value - high.astype(jnp.float32)).astype(jnp.bfloat16)
    return high, low


def thirds(value):
    high = value.astype(jnp.bfloat16)
    rest = value - high.astype(jnp.float32)
    middle, low = split(rest)
    return high, middle, low


def nt(left, right, precision=None):
    return lax.dot_general(
        left, right, (((1,), (1,)), ((), ())), precision=precision, preferred_element_type=jnp.float32
    )


def nn(left, right, precision=None):
    return lax.dot_general(
        left, right, (((1,), (0,)), ((), ())), precision=precision, preferred_element_type=jnp.float32
    )


def nn_six(left, right):
    lh, lm, ll = thirds(left)
    rh, rm, rl = thirds(right)
    small = nn(lm, rm) + nn(lh, rl) + nn(ll, rh)
    return nn(lh, rh) + (nn(lh, rm) + nn(lm, rh) + small)


def inverse_factor(gram):
    n = gram.shape[0]
    rows = lax.broadcasted_iota(jnp.int32, (n, n), 0)
    cols = lax.broadcasted_iota(jnp.int32, (n, n), 1)
    work = gram
    inverse = jnp.where(rows == cols, 1.0, 0.0).astype(jnp.float32)
    pivots = jnp.ones((n, n), jnp.float32)
    for j in range(0, n, GROUP):
        columns = [jnp.broadcast_to(work[:, j + p : j + p + 1], (n, n)) for p in range(GROUP)]
        lines = [work[j + p : j + p + 1, :] for p in range(GROUP)]
        others = [inverse[j + p : j + p + 1, :] for p in range(GROUP)]
        for p in range(GROUP):
            pivot = columns[p][j + p : j + p + 1, :]
            reciprocal = 1.0 / pivot
            pivots = jnp.where(rows == j + p, pivot, pivots)
            for q in range(p + 1, GROUP):
                weight = columns[p][j + q : j + q + 1, :] * reciprocal
                columns[q] = columns[q] - columns[p] * weight
                lines[q] = lines[q] - lines[p] * weight
                others[q] = others[q] - others[p] * weight
            lines[p] = lines[p] * reciprocal
            others[p] = others[p] * reciprocal
            columns[p] = jnp.where(rows > j + p, columns[p], 0.0)
        for p in range(GROUP):
            inverse = inverse - columns[p] * others[p]
            if j + GROUP < n:
                work = work - columns[p] * lines[p]
    return inverse / jnp.sqrt(pivots)


def kernel(
    row_size, col_size, coefs_ref, tilts_ref, basis_ref, ccc_ref, out_ref,
    xall, start, first, keep, energy, xh, xl, eh, el, mb, part, rx_pair, rx_plane, rx_row, packed, ch, cl,
    own_sem, x_send, x_recv, v_send, v_recv, pair_send, pair_recv, plane_send, plane_recv,
    row_send, row_recv, zg_send, zg_recv, cg_send, cg_recv,
):
    z = lax.axis_index("row")
    c = lax.axis_index("col")
    rows = coefs_ref.shape[1]
    width = coefs_ref.shape[2]
    total = rows * row_size
    piece = width // row_size
    eig, basis_rows = basis_ref.shape
    chunks = piece // TILE
    size = total // BLOCKS

    barrier = pltpu.get_barrier_semaphore()
    for mask in range(1, row_size):
        pl.semaphore_signal(barrier, inc=1, device_id={"row": flip(z, mask)}, device_id_type=MESH)
    for mask in range(1, col_size):
        pl.semaphore_signal(barrier, inc=1, device_id={"col": flip(c, mask)}, device_id_type=MESH)
    pl.semaphore_wait(barrier, row_size + col_size - 2)

    def remote(source, target, send, recv, mask, axis):
        other = flip(z if axis == "row" else c, mask)
        return pltpu.make_async_remote_copy(
            src_ref=source, dst_ref=target, send_sem=send.at[mask - 1], recv_sem=recv.at[mask - 1],
            device_id={axis: other}, device_id_type=MESH,
        )

    own_rows = pl.ds(pl.multiple_of(z * rows, 8), rows)
    exchange = {}
    for q in range(chunks):
        here = pl.ds(q * TILE, TILE)
        for mask in far_first(row_size):
            lanes = pl.ds(pl.multiple_of(flip(z, mask) * piece + q * TILE, TILE), TILE)
            slot = q * (row_size - 1) + mask - 1
            exchange[q, mask] = pltpu.make_async_remote_copy(
                src_ref=coefs_ref.at[:, :, lanes], dst_ref=xall.at[:, own_rows, here],
                send_sem=x_send.at[slot], recv_sem=x_recv.at[slot],
                device_id={"row": flip(z, mask)}, device_id_type=MESH,
            )
            exchange[q, mask].start()
    own = pltpu.make_async_copy(
        coefs_ref.at[:, :, pl.ds(pl.multiple_of(z * piece, TILE), piece)], xall.at[:, own_rows, :], own_sem
    )
    own.start()
    start[c] = basis_ref[...]
    starts = []
    for mask in range(1, col_size):
        copy = remote(basis_ref, start.at[c], v_send, v_recv, mask, "col")
        copy.start()
        starts.append(copy)

    wave = c * width + z * piece + lax.broadcasted_iota(jnp.int32, (TILE, TILE), 1)
    wave_x = jnp.abs(wave // (GRID * (GRID // 2)) - GRID // 2).astype(jnp.float32)
    wave_z = (wave % GRID - GRID // 2).astype(jnp.float32) * 16.0
    for i in range(0, total, TILE):
        limits = tilts_ref[:, i : i + TILE].astype(jnp.float32)
        below = jnp.broadcast_to(limits[0:1, :], (TILE, TILE)).T
        above = jnp.broadcast_to(limits[1:2, :], (TILE, TILE)).T
        inside = jnp.where(wave_z >= 0, wave_z - above * wave_x, -wave_z - below * wave_x) <= 0
        mask = jnp.where(inside, 1.0, 0.0)
        keep[i : i + TILE, :] = mask
        mb[i : i + TILE, :] = mask.astype(jnp.bfloat16)

    for copy in starts:
        copy.wait()
    places = lax.broadcasted_iota(jnp.int32, (basis_rows, total), 1) - lax.broadcasted_iota(
        jnp.int32, (basis_rows, total), 0
    )
    for k in range(col_size):
        term = nn(start[k], jnp.where(places == k * basis_rows, 1.0, 0.0).astype(jnp.float32), HIGH)
        first[...] = term if k == 0 else first[...] + term

    def prepare(q, index):
        span = pl.ds(pl.multiple_of(index * rows, 16), rows)
        lanes = slice(q * TILE, (q + 1) * TILE)
        mask = keep[span, :]
        real = xall[0, span, lanes] * mask
        imag = xall[1, span, lanes] * mask
        for part_lanes, value in ((slice(2 * q * TILE, (2 * q + 1) * TILE), real), (slice((2 * q + 1) * TILE, (2 * q + 2) * TILE), imag)):
            xh[span, part_lanes], xl[span, part_lanes] = split(value)
        power = real * real + imag * imag
        if q > 0:
            power = power + energy[span, :]
        if q < chunks - 1:
            energy[span, :] = power
        else:
            eh[span, :], el[span, :] = split(power)

    def products(q):
        lanes = slice(2 * q * TILE, 2 * (q + 1) * TILE)
        for a in range(BLOCKS):
            for t in range(2):
                b = (a + t) % BLOCKS
                right = slice(b * size, (b + 1) * size)
                out = slice(t * size, (t + 1) * size)

                def tile(index, carry, a=a, right=right, out=out):
                    left = pl.ds(pl.multiple_of(a * size + index * TILE, TILE), TILE)
                    value = (
                        nt(xh[left, lanes], xh[right, lanes])
                        + nt(xh[left, lanes], xl[right, lanes])
                        + nt(xl[left, lanes], xh[right, lanes])
                    )
                    part[0, left, out] = value if q == 0 else part[0, left, out] + value
                    if q == chunks - 1:
                        part[1, left, out] = nt(eh[left, :], mb[right, :]) + nt(el[left, :], mb[right, :])
                        part[2, left, out] = nt(mb[left, :], eh[right, :]) + nt(mb[left, :], el[right, :])
                    return carry

                lax.fori_loop(0, size // TILE, tile, 0)

    own.wait()
    for q in range(chunks):
        prepare(q, z)
        for mask in far_first(row_size):
            exchange[q, mask].wait()
            prepare(q, flip(z, mask))
        products(q)

    pairs = col_size // 2
    side = c % 2
    half = total // 2
    strip = total // col_size
    theirs = pl.ds(pl.multiple_of((1 - side) * half, 8), half)
    mine = pl.ds(pl.multiple_of(side * half, 8), half)
    pair = remote(part.at[:, theirs, :], rx_pair, pair_send, pair_recv, 1, "col")
    pair.start()
    pair.wait()
    part[:, mine, :] = part[:, mine, :] + rx_pair[...]
    group = c // 2
    copies = []
    for mask in far_first(pairs):
        there = pl.ds(pl.multiple_of(side * half + flip(group, mask) * strip, 8), strip)
        copy = pltpu.make_async_remote_copy(
            src_ref=part.at[:, there, :], dst_ref=rx_plane.at[mask - 1],
            send_sem=plane_send.at[mask - 1], recv_sem=plane_recv.at[mask - 1],
            device_id={"col": flip(c, 2 * mask)}, device_id_type=MESH,
        )
        copy.start()
        copies.append(copy)
    for copy in copies:
        copy.wait()
    base = side * half + group * strip
    strip_rows = pl.ds(pl.multiple_of(base, 8), strip)
    part[:, strip_rows, :] = part[:, strip_rows, :] + sum(rx_plane[k] for k in range(pairs - 1))

    cuts = row_size // 2
    short = strip // cuts

    def region(index):
        return (
            pl.ds(pl.multiple_of(base + (index // 2) * short, 8), short),
            pl.ds(pl.multiple_of((index % 2) * size, TILE), size),
        )

    copies = []
    for mask in far_first(row_size):
        there = region(flip(z, mask))
        copy = remote(part.at[:, there[0], there[1]], rx_row.at[mask - 1], row_send, row_recv, mask, "row")
        copy.start()
        copies.append(copy)
    for copy in copies:
        copy.wait()
    here = region(z)
    sums = part[:, here[0], here[1]] + sum(rx_row[k] for k in range(row_size - 1))
    packed[here[0], here[1]] = sums[0] / jnp.sqrt(sums[1] * sums[2] + EPS)

    copies = []
    for mask in far_first(row_size):
        spot = packed.at[here[0], here[1]]
        copy = remote(spot, spot, zg_send, zg_recv, mask, "row")
        copy.start()
        copies.append(copy)
    for copy in copies:
        copy.wait()
    copies = []
    for mask in far_first(col_size):
        spot = packed.at[strip_rows, :]
        copy = remote(spot, spot, cg_send, cg_recv, mask, "col")
        copy.start()
        copies.append(copy)
    for copy in copies:
        copy.wait()

    def place(i, j, value):
        down, across = slice(i, i + TILE), slice(j, j + TILE)
        plane, lane = (0, j) if j < 2 * size else (1, j - 2 * size)
        part[plane, down, lane : lane + TILE] = value
        ch[down, across], cl[down, across] = split(value)

    for a in range(BLOCKS):
        for t in range(2):
            b = (a + t) % BLOCKS
            for i in range(0, size, TILE):
                for j in range(0, size, TILE):
                    block = packed[a * size + i : a * size + i + TILE, t * size + j : t * size + j + TILE]
                    place(a * size + i, b * size + j, block)
                    if t:
                        place(b * size + j, a * size + i, block.T)

    chosen = lax.broadcasted_iota(jnp.int32, (basis_rows, total), 1)
    chosen = chosen == c * basis_rows + lax.broadcasted_iota(jnp.int32, (basis_rows, total), 0)
    chosen = jnp.where(chosen, 1.0, 0.0).astype(jnp.float32)
    ccc_ref[...] = nt(chosen[:, : 2 * size], part[0, own_rows, :], HIGH) + nt(
        chosen[:, 2 * size :], part[1, own_rows, :size], HIGH
    )

    def iterate(step, current):
        high, low = split(current)
        wide = nn(high, ch[...]) + nn(high, cl[...]) + nn(low, ch[...])
        return nn_six(inverse_factor(nt(wide, wide, HIGH)), wide)

    last = first[...]
    for step in range(ITERS):
        last = iterate(step, last)
    out_ref[...] = nt(last, chosen, HIGH) * math.sqrt(total)


def local(coefs, tilts, start_basis):
    row_size = lax.axis_size("row")
    col_size = lax.axis_size("col")
    rows, width = coefs.shape[1:]
    basis_rows, eig = start_basis.shape
    total = rows * row_size
    piece = width // row_size
    lanes = 2 * (total // BLOCKS)
    strip = total // col_size
    pairs = col_size // 2
    f32, b16 = jnp.float32, jnp.bfloat16
    dma = lambda n: pltpu.SemaphoreType.DMA((n,))
    vmem = pl.BlockSpec(memory_space=pltpu.VMEM)
    ccc, basis = pl.pallas_call(
        functools.partial(kernel, row_size, col_size),
        out_shape=(
            jax.ShapeDtypeStruct((basis_rows, rows), f32),
            jax.ShapeDtypeStruct((eig, basis_rows), f32),
        ),
        in_specs=[pl.BlockSpec(memory_space=pl.ANY), vmem, vmem],
        out_specs=(vmem, vmem),
        scratch_shapes=[
            pltpu.VMEM((2, total, piece), f32),
            pltpu.VMEM((col_size, eig, basis_rows), f32),
            pltpu.VMEM((eig, total), f32),
            pltpu.VMEM((total, TILE), f32),
            pltpu.VMEM((total, TILE), f32),
            pltpu.VMEM((total, 2 * piece), b16),
            pltpu.VMEM((total, 2 * piece), b16),
            pltpu.VMEM((total, TILE), b16),
            pltpu.VMEM((total, TILE), b16),
            pltpu.VMEM((total, TILE), b16),
            pltpu.VMEM((3, total, lanes), f32),
            pltpu.VMEM((3, total // 2, lanes), f32),
            pltpu.VMEM((pairs - 1, 3, strip, lanes), f32),
            pltpu.VMEM((row_size - 1, 3, strip // (row_size // 2), lanes // 2), f32),
            pltpu.VMEM((total, lanes), f32),
            pltpu.VMEM((total, total), b16),
            pltpu.VMEM((total, total), b16),
            pltpu.SemaphoreType.DMA,
            dma(piece // TILE * (row_size - 1)), dma(piece // TILE * (row_size - 1)),
            dma(col_size - 1), dma(col_size - 1),
            dma(1), dma(1),
            dma(pairs - 1), dma(pairs - 1),
            dma(row_size - 1), dma(row_size - 1),
            dma(row_size - 1), dma(row_size - 1),
            dma(col_size - 1), dma(col_size - 1),
        ],
        compiler_params=pltpu.CompilerParams(
            collective_id=0, has_side_effects=True, vmem_limit_bytes=67043328
        ),
        name="subspace",
    )(coefs, tilts.T, start_basis.T)
    return ccc.T, basis.T


def solution(mesh):
    in_specs = (P(None, "row", "col"), P(), P("col", None))
    out_specs = (P("row", "col"), P("col", None))
    return jax.shard_map(local, mesh=mesh, in_specs=in_specs, out_specs=out_specs, check_vma=False)
```

```python
import functools
import math

import jax
import jax.numpy as jnp
from jax import lax
from jax.experimental import pallas as pl
from jax.experimental.pallas import tpu as pltpu
from jax.sharding import PartitionSpec as P

GRID = 32
ITERS = 4
EPS = 1e-06
HIGH = lax.Precision.HIGHEST
MESH = pl.DeviceIdType.MESH
TILE = 128
BLOCKS = 3
GROUP = 8


def flip(index, mask):
    out = index
    bit = 1
    while bit <= mask:
        if mask & bit:
            out = out + bit * (1 - 2 * ((index // bit) % 2))
        bit *= 2
    return out


def far_first(count):
    return sorted(range(1, count), key=lambda mask: (-mask.bit_length(), mask))


def split(value):
    high = value.astype(jnp.bfloat16)
    low = (value - high.astype(jnp.float32)).astype(jnp.bfloat16)
    return high, low


def thirds(value):
    high = value.astype(jnp.bfloat16)
    rest = value - high.astype(jnp.float32)
    middle, low = split(rest)
    return high, middle, low


def nt(left, right, precision=None):
    return lax.dot_general(
        left, right, (((1,), (1,)), ((), ())), precision=precision, preferred_element_type=jnp.float32
    )


def nn(left, right, precision=None):
    return lax.dot_general(
        left, right, (((1,), (0,)), ((), ())), precision=precision, preferred_element_type=jnp.float32
    )


def nn_six(left, right):
    lh, lm, ll = thirds(left)
    rh, rm, rl = thirds(right)
    small = nn(lm, rm) + nn(lh, rl) + nn(ll, rh)
    return nn(lh, rh) + (nn(lh, rm) + nn(lm, rh) + small)


def inverse_factor(gram):
    n = gram.shape[0]
    rows = lax.broadcasted_iota(jnp.int32, (n, n), 0)
    cols = lax.broadcasted_iota(jnp.int32, (n, n), 1)
    work = gram
    inverse = jnp.where(rows == cols, 1.0, 0.0).astype(jnp.float32)
    pivots = jnp.ones((n, n), jnp.float32)
    for j in range(0, n, GROUP):
        columns = [jnp.broadcast_to(work[:, j + p : j + p + 1], (n, n)) for p in range(GROUP)]
        lines = [work[j + p : j + p + 1, :] for p in range(GROUP)]
        others = [inverse[j + p : j + p + 1, :] for p in range(GROUP)]
        for p in range(GROUP):
            pivot = columns[p][j + p : j + p + 1, :]
            reciprocal = 1.0 / pivot
            pivots = jnp.where(rows == j + p, pivot, pivots)
            for q in range(p + 1, GROUP):
                weight = columns[p][j + q : j + q + 1, :] * reciprocal
                columns[q] = columns[q] - columns[p] * weight
                lines[q] = lines[q] - lines[p] * weight
                others[q] = others[q] - others[p] * weight
            lines[p] = lines[p] * reciprocal
            others[p] = others[p] * reciprocal
            columns[p] = jnp.where(rows > j + p, columns[p], 0.0)
        for p in range(GROUP):
            inverse = inverse - columns[p] * others[p]
            if j + GROUP < n:
                work = work - columns[p] * lines[p]
    return inverse / jnp.sqrt(pivots)


def kernel(
    row_size, col_size, coefs_ref, tilts_ref, basis_ref, ccc_ref, out_ref,
    xall, start, first, keep, energy, xh, xl, eh, el, mb, part, rx_pair, rx_plane, rx_row, packed, ch, cl,
    own_sem, x_send, x_recv, v_send, v_recv, pair_send, pair_recv, plane_send, plane_recv,
    row_send, row_recv, zg_send, zg_recv, cg_send, cg_recv,
):
    z = lax.axis_index("row")
    c = lax.axis_index("col")
    rows = coefs_ref.shape[1]
    width = coefs_ref.shape[2]
    total = rows * row_size
    piece = width // row_size
    eig, basis_rows = basis_ref.shape
    chunks = piece // TILE
    size = total // BLOCKS

    barrier = pltpu.get_barrier_semaphore()
    for mask in range(1, row_size):
        pl.semaphore_signal(barrier, inc=1, device_id={"row": flip(z, mask)}, device_id_type=MESH)
    for mask in range(1, col_size):
        pl.semaphore_signal(barrier, inc=1, device_id={"col": flip(c, mask)}, device_id_type=MESH)
    pl.semaphore_wait(barrier, row_size + col_size - 2)

    def remote(source, target, send, recv, mask, axis):
        other = flip(z if axis == "row" else c, mask)
        return pltpu.make_async_remote_copy(
            src_ref=source, dst_ref=target, send_sem=send.at[mask - 1], recv_sem=recv.at[mask - 1],
            device_id={axis: other}, device_id_type=MESH,
        )

    own_rows = pl.ds(pl.multiple_of(z * rows, 8), rows)
    exchange = {}
    for q in range(chunks):
        here = pl.ds(q * TILE, TILE)
        for mask in far_first(row_size):
            lanes = pl.ds(pl.multiple_of(flip(z, mask) * piece + q * TILE, TILE), TILE)
            slot = q * (row_size - 1) + mask - 1
            exchange[q, mask] = pltpu.make_async_remote_copy(
                src_ref=coefs_ref.at[:, :, lanes], dst_ref=xall.at[:, own_rows, here],
                send_sem=x_send.at[slot], recv_sem=x_recv.at[slot],
                device_id={"row": flip(z, mask)}, device_id_type=MESH,
            )
            exchange[q, mask].start()
    own = pltpu.make_async_copy(
        coefs_ref.at[:, :, pl.ds(pl.multiple_of(z * piece, TILE), piece)], xall.at[:, own_rows, :], own_sem
    )
    own.start()
    start[c] = basis_ref[...]
    starts = []
    for mask in range(1, col_size):
        copy = remote(basis_ref, start.at[c], v_send, v_recv, mask, "col")
        copy.start()
        starts.append(copy)

    wave = c * width + z * piece + lax.broadcasted_iota(jnp.int32, (TILE, TILE), 1)
    wave_x = jnp.abs(wave // (GRID * (GRID // 2)) - GRID // 2).astype(jnp.float32)
    wave_z = (wave % GRID - GRID // 2).astype(jnp.float32) * 16.0
    for i in range(0, total, TILE):
        limits = tilts_ref[:, i : i + TILE].astype(jnp.float32)
        below = jnp.broadcast_to(limits[0:1, :], (TILE, TILE)).T
        above = jnp.broadcast_to(limits[1:2, :], (TILE, TILE)).T
        inside = jnp.where(wave_z >= 0, wave_z - above * wave_x, -wave_z - below * wave_x) <= 0
        mask = jnp.where(inside, 1.0, 0.0)
        keep[i : i + TILE, :] = mask
        mb[i : i + TILE, :] = mask.astype(jnp.bfloat16)

    for copy in starts:
        copy.wait()
    places = lax.broadcasted_iota(jnp.int32, (basis_rows, total), 1) - lax.broadcasted_iota(
        jnp.int32, (basis_rows, total), 0
    )
    for k in range(col_size):
        term = nn(start[k], jnp.where(places == k * basis_rows, 1.0, 0.0).astype(jnp.float32), HIGH)
        first[...] = term if k == 0 else first[...] + term

    def prepare(q, index):
        span = pl.ds(pl.multiple_of(index * rows, 16), rows)
        lanes = slice(q * TILE, (q + 1) * TILE)
        mask = keep[span, :]
        real = xall[0, span, lanes] * mask
        imag = xall[1, span, lanes] * mask
        for part_lanes, value in ((slice(2 * q * TILE, (2 * q + 1) * TILE), real), (slice((2 * q + 1) * TILE, (2 * q + 2) * TILE), imag)):
            xh[span, part_lanes], xl[span, part_lanes] = split(value)
        power = real * real + imag * imag
        if q > 0:
            power = power + energy[span, :]
        if q < chunks - 1:
            energy[span, :] = power
        else:
            eh[span, :], el[span, :] = split(power)

    def blocks(write):
        for a in range(BLOCKS):
            for t in range(2):
                b = (a + t) % BLOCKS
                right = slice(b * size, (b + 1) * size)
                out = slice(t * size, (t + 1) * size)

                def tile(index, carry, a=a, right=right, out=out):
                    write(pl.ds(pl.multiple_of(a * size + index * TILE, TILE), TILE), right, out)
                    return carry

                lax.fori_loop(0, size // TILE, tile, 0)

    def intersections(left, right, out):
        part[1, left, out] = nt(eh[left, :], mb[right, :]) + nt(el[left, :], mb[right, :])
        part[2, left, out] = nt(mb[left, :], eh[right, :]) + nt(mb[left, :], el[right, :])

    def numerators(q, left, right, out):
        lanes = slice(2 * q * TILE, 2 * (q + 1) * TILE)
        value = (
            nt(xh[left, lanes], xh[right, lanes])
            + nt(xh[left, lanes], xl[right, lanes])
            + nt(xl[left, lanes], xh[right, lanes])
        )
        part[0, left, out] = value if q == 0 else part[0, left, out] + value

    pairs = col_size // 2
    side = c % 2
    half = total // 2
    strip = total // col_size
    group = c // 2
    theirs = pl.ds(pl.multiple_of((1 - side) * half, 8), half)
    mine = pl.ds(pl.multiple_of(side * half, 8), half)
    planes = (slice(1, 3), slice(0, 1))

    def pair_copy(turn):
        return pltpu.make_async_remote_copy(
            src_ref=part.at[planes[turn], theirs, :], dst_ref=rx_pair.at[planes[turn]],
            send_sem=pair_send.at[turn], recv_sem=pair_recv.at[turn],
            device_id={"col": flip(c, 1)}, device_id_type=MESH,
        )

    def plane_copy(turn, mask):
        there = pl.ds(pl.multiple_of(side * half + flip(group, mask) * strip, 8), strip)
        slot = turn * (pairs - 1) + mask - 1
        return pltpu.make_async_remote_copy(
            src_ref=part.at[planes[turn], there, :], dst_ref=rx_plane.at[mask - 1, planes[turn]],
            send_sem=plane_send.at[slot], recv_sem=plane_recv.at[slot],
            device_id={"col": flip(c, 2 * mask)}, device_id_type=MESH,
        )

    own.wait()
    for q in range(chunks):
        prepare(q, z)
        for mask in far_first(row_size):
            exchange[q, mask].wait()
            prepare(q, flip(z, mask))
        if q < chunks - 1:
            blocks(functools.partial(numerators, q))
    blocks(intersections)
    pair = [pair_copy(turn) for turn in range(2)]
    pair[0].start()
    blocks(functools.partial(numerators, chunks - 1))
    pair[1].start()
    copies = []
    for turn in range(2):
        pair[turn].wait()
        part[planes[turn], mine, :] = part[planes[turn], mine, :] + rx_pair[planes[turn]]
        for mask in far_first(pairs):
            copies.append(plane_copy(turn, mask))
            copies[-1].start()
    for copy in copies:
        copy.wait()

    base = side * half + group * strip
    strip_rows = pl.ds(pl.multiple_of(base, 8), strip)
    part[:, strip_rows, :] = part[:, strip_rows, :] + sum(rx_plane[k] for k in range(pairs - 1))

    cuts = row_size // 2
    short = strip // cuts

    def region(index):
        return (
            pl.ds(pl.multiple_of(base + (index // 2) * short, 8), short),
            pl.ds(pl.multiple_of((index % 2) * size, TILE), size),
        )

    copies = []
    for mask in far_first(row_size):
        there = region(flip(z, mask))
        copy = remote(part.at[:, there[0], there[1]], rx_row.at[mask - 1], row_send, row_recv, mask, "row")
        copy.start()
        copies.append(copy)
    for copy in copies:
        copy.wait()
    here = region(z)
    sums = part[:, here[0], here[1]] + sum(rx_row[k] for k in range(row_size - 1))
    packed[here[0], here[1]] = sums[0] / jnp.sqrt(sums[1] * sums[2] + EPS)

    copies = []
    for mask in far_first(row_size):
        spot = packed.at[here[0], here[1]]
        copy = remote(spot, spot, zg_send, zg_recv, mask, "row")
        copy.start()
        copies.append(copy)
    for copy in copies:
        copy.wait()
    copies = []
    for mask in far_first(col_size):
        spot = packed.at[strip_rows, :]
        copy = remote(spot, spot, cg_send, cg_recv, mask, "col")
        copy.start()
        copies.append(copy)
    for copy in copies:
        copy.wait()

    def place(i, j, value):
        down, across = slice(i, i + TILE), slice(j, j + TILE)
        plane, lane = (0, j) if j < 2 * size else (1, j - 2 * size)
        part[plane, down, lane : lane + TILE] = value
        ch[down, across], cl[down, across] = split(value)

    for a in range(BLOCKS):
        for t in range(2):
            b = (a + t) % BLOCKS
            for i in range(0, size, TILE):
                for j in range(0, size, TILE):
                    block = packed[a * size + i : a * size + i + TILE, t * size + j : t * size + j + TILE]
                    place(a * size + i, b * size + j, block)
                    if t:
                        place(b * size + j, a * size + i, block.T)

    chosen = lax.broadcasted_iota(jnp.int32, (basis_rows, total), 1)
    chosen = chosen == c * basis_rows + lax.broadcasted_iota(jnp.int32, (basis_rows, total), 0)
    chosen = jnp.where(chosen, 1.0, 0.0).astype(jnp.float32)
    ccc_ref[...] = nt(chosen[:, : 2 * size], part[0, own_rows, :], HIGH) + nt(
        chosen[:, 2 * size :], part[1, own_rows, :size], HIGH
    )

    def iterate(step, current):
        high, low = split(current)
        wide = nn(high, ch[...]) + nn(high, cl[...]) + nn(low, ch[...])
        return nn_six(inverse_factor(nt(wide, wide, HIGH)), wide)

    last = first[...]
    for step in range(ITERS):
        last = iterate(step, last)
    out_ref[...] = nt(last, chosen, HIGH) * math.sqrt(total)


def local(coefs, tilts, start_basis):
    row_size = lax.axis_size("row")
    col_size = lax.axis_size("col")
    rows, width = coefs.shape[1:]
    basis_rows, eig = start_basis.shape
    total = rows * row_size
    piece = width // row_size
    lanes = 2 * (total // BLOCKS)
    strip = total // col_size
    pairs = col_size // 2
    f32, b16 = jnp.float32, jnp.bfloat16
    dma = lambda n: pltpu.SemaphoreType.DMA((n,))
    vmem = pl.BlockSpec(memory_space=pltpu.VMEM)
    ccc, basis = pl.pallas_call(
        functools.partial(kernel, row_size, col_size),
        out_shape=(
            jax.ShapeDtypeStruct((basis_rows, rows), f32),
            jax.ShapeDtypeStruct((eig, basis_rows), f32),
        ),
        in_specs=[pl.BlockSpec(memory_space=pl.ANY), vmem, vmem],
        out_specs=(vmem, vmem),
        scratch_shapes=[
            pltpu.VMEM((2, total, piece), f32),
            pltpu.VMEM((col_size, eig, basis_rows), f32),
            pltpu.VMEM((eig, total), f32),
            pltpu.VMEM((total, TILE), f32),
            pltpu.VMEM((total, TILE), f32),
            pltpu.VMEM((total, 2 * piece), b16),
            pltpu.VMEM((total, 2 * piece), b16),
            pltpu.VMEM((total, TILE), b16),
            pltpu.VMEM((total, TILE), b16),
            pltpu.VMEM((total, TILE), b16),
            pltpu.VMEM((3, total, lanes), f32),
            pltpu.VMEM((3, total // 2, lanes), f32),
            pltpu.VMEM((pairs - 1, 3, strip, lanes), f32),
            pltpu.VMEM((row_size - 1, 3, strip // (row_size // 2), lanes // 2), f32),
            pltpu.VMEM((total, lanes), f32),
            pltpu.VMEM((total, total), b16),
            pltpu.VMEM((total, total), b16),
            pltpu.SemaphoreType.DMA,
            dma(piece // TILE * (row_size - 1)), dma(piece // TILE * (row_size - 1)),
            dma(col_size - 1), dma(col_size - 1),
            dma(2), dma(2),
            dma(2 * (pairs - 1)), dma(2 * (pairs - 1)),
            dma(row_size - 1), dma(row_size - 1),
            dma(row_size - 1), dma(row_size - 1),
            dma(col_size - 1), dma(col_size - 1),
        ],
        compiler_params=pltpu.CompilerParams(
            collective_id=0, has_side_effects=True, vmem_limit_bytes=67043328
        ),
        name="subspace",
    )(coefs, tilts.T, start_basis.T)
    return ccc.T, basis.T


def solution(mesh):
    in_specs = (P(None, "row", "col"), P(), P("col", None))
    out_specs = (P("row", "col"), P("col", None))
    return jax.shard_map(local, mesh=mesh, in_specs=in_specs, out_specs=out_specs, check_vma=False)
```
